32 devices in a mesh: sta: 8 (over z, y), seg: 4 (over x, core).
Axes of the slice: x: 2, y: 2, z: 4, core: 2. Of those that a mesh axis runs over, the one named last changes fastest.
Arguments:
- spectra: bfloat16 [2, 8, 512, 4096], P(None, 'seg', None, 'sta'), may hold values from -6 to 6
- bin_index: int32 [512], replicated, may hold values from 0 to 4096
Outputs:
- correlation: float32 [2, 4096, 4096], P(None, ('sta', 'seg'))
The draws below stay inside these ranges and needn't reach their ends.
All inputs are finite; a program needn't handle non-finite values.
Results may differ from the reference program's by a relative error of at most 0.012.
Values may be sent and summed in bfloat16 or wider, within the bound.
A program may use at most 64 MiB of HBM per device.

```python
import math
import jax
import jax.numpy as jnp
from jax import lax

S = 4096
NFFT = 8192
F = 512
SEG_DEV = 2
LAGS = 2
LAG_STEP = 37
HALF = 64
SEGMENTS = 8
N_SEG = 4


def with_ends(array, own_key, low, top_value):
    shape = array.shape
    index_at = [jax.random.randint(jax.random.fold_in(own_key, axis), (), 0, shape[axis]) for axis in range(len(shape))]
    array = array.at[tuple(index_at)].set(low)
    longest = shape.index(max(shape))
    index_at[longest] = (index_at[longest] + 1) % shape[longest]
    return array.at[tuple(index_at)].set(top_value)


def level_of(key, extent, pieces, least, high):
    def one(position, parts):
        draws = jax.random.uniform(jax.random.fold_in(jax.random.fold_in(key, 6), position), (parts,), jnp.float32, least / len(pieces), high / len(pieces))
        return jnp.repeat(jnp.exp(draws), extent[position] // parts).reshape((-1,) + (1,) * (len(extent) - position - 1))

    loudness = one(*pieces[0])
    for cut in pieces[1:]:
        loudness = loudness * one(*cut)
    return loudness


def gaussian(rng, dims, width, limit, pieces=(), kind=jnp.bfloat16):
    result = jax.random.normal(rng, dims, jnp.float32) * width
    if len(pieces) > 0:
        result = level_of(rng, dims, pieces, -0.22, 0.18) * result
    return jnp.clip(result, min=-limit, max=limit).astype(kind)


def setup_inputs(seed: int = 0) -> dict:
    keys = jax.random.split(jax.random.key(seed), 3)
    spectra = gaussian(keys[0], (2, SEGMENTS, F, S), 1.0, 6.0, ((1, 4), (3, 8)))
    bin_index = with_ends(jax.random.randint(keys[1], (F,), 0, NFFT // 2 + 1), jax.random.fold_in(keys[1], 1), 0, (NFFT // 2 + 1) - 1).astype(jnp.int32)
    return {"spectra": spectra, "bin_index": bin_index}


def whiten(spectra):
    values = spectra.astype(jnp.float32)
    energy = values[0] * values[0] + values[1] * values[1]
    freq_bins = values.shape[2]
    bin_pos = jnp.arange(freq_bins, dtype=jnp.int32)
    window = (jnp.abs(bin_pos[:, None] - bin_pos[None, :]) <= HALF).astype(jnp.float32)
    bin_count = lax.optimization_barrier(jnp.sum(window, axis=1))
    smoothed = jnp.einsum('gf,sfc->sgc', window, energy, precision=lax.Precision.HIGHEST) / bin_count[None, :, None]
    return (values / jnp.sqrt(smoothed + 1e-06)[None]).astype(jnp.bfloat16)

def phases(bin_index):
    lag_samples = (jnp.arange(LAGS, dtype=jnp.int32) + 1) * LAG_STEP
    phase_turn = lag_samples[:, None] * bin_index[None, :].astype(jnp.int32) % NFFT
    phase_angle = 2.0 * math.pi / NFFT * phase_turn.astype(jnp.float32)
    return (jnp.cos(phase_angle), jnp.sin(phase_angle))

def rotate(whitened, cosine, sine_part):
    real_part = whitened[0].astype(jnp.float32)[None]
    imag_part = whitened[1].astype(jnp.float32)[None]
    cos_part = cosine[:, None, :, None]
    sin_part = sine_part[:, None, :, None]
    rot_real = real_part * cos_part - imag_part * sin_part
    rot_imag = real_part * sin_part + imag_part * cos_part
    stacked = jnp.stack([rot_real, rot_imag], axis=1).astype(jnp.bfloat16)
    return stacked.reshape(cosine.shape[0], -1, whitened.shape[3])

def reference(spectra, bin_index):
    whitened = whiten(spectra)
    cosine, sine_part = phases(bin_index)
    norm_scale = 1.0 / math.sqrt(SEGMENTS * F)
    stations = whitened.shape[3]

    def add_group(group_idx, total):
        first_seg = (group_idx * SEG_DEV).astype(jnp.int32)
        group_spec = lax.dynamic_slice_in_dim(whitened, first_seg, SEG_DEV, 1)
        rotated = rotate(group_spec, cosine, sine_part).astype(jnp.float32)
        columns = group_spec.reshape(-1, stations).astype(jnp.float32)
        product = jnp.einsum('mki,kj->mij', rotated, columns, precision=lax.Precision.HIGHEST)
        stacked = lax.optimization_barrier((product * norm_scale).astype(jnp.bfloat16))
        return total + stacked.astype(jnp.float32)
    zero_total = jnp.zeros((LAGS, stations, stations), jnp.float32)
    return lax.fori_loop(0, N_SEG, add_group, zero_total)
```

```python
import math

import jax
import jax.numpy as jnp
from jax import lax
from jax.sharding import PartitionSpec as P

NFFT = 8192
LAGS = 2
LAG_STEP = 37
HALF = 64


def whiten(spectra):
    values = spectra.astype(jnp.float32)
    energy = values[0] * values[0] + values[1] * values[1]
    freq_bins = values.shape[2]
    bin_pos = jnp.arange(freq_bins, dtype=jnp.int32)
    window = (jnp.abs(bin_pos[:, None] - bin_pos[None, :]) <= HALF).astype(jnp.float32)
    bin_count = jnp.sum(window, axis=1)
    smoothed = (
        jnp.einsum("gf,sfc->sgc", window, energy, precision=lax.Precision.HIGHEST)
        / bin_count[None, :, None]
    )
    return (values / jnp.sqrt(smoothed + 1e-06)[None]).astype(jnp.bfloat16)


def phases(bin_index):
    lag_samples = (jnp.arange(LAGS, dtype=jnp.int32) + 1) * LAG_STEP
    phase_turn = lag_samples[:, None] * bin_index[None, :] % NFFT
    phase_angle = 2.0 * math.pi / NFFT * phase_turn.astype(jnp.float32)
    return (jnp.cos(phase_angle), jnp.sin(phase_angle))


def rotate(whitened, cosine, sine_part):
    real_part = whitened[0].astype(jnp.float32)[None]
    imag_part = whitened[1].astype(jnp.float32)[None]
    cos_part = cosine[:, None, :, None]
    sin_part = sine_part[:, None, :, None]
    rot_real = real_part * cos_part - imag_part * sin_part
    rot_imag = real_part * sin_part + imag_part * cos_part
    stacked = jnp.stack([rot_real, rot_imag], axis=1).astype(jnp.bfloat16)
    return stacked.reshape(cosine.shape[0], -1, whitened.shape[3])


def pair_block(rotated, columns, norm_scale):
    product = jnp.einsum("mki,kj->mij", rotated, columns, preferred_element_type=jnp.float32)
    return (product * norm_scale).astype(jnp.bfloat16)


def general_body(spectra, bin_index):
    whitened = whiten(spectra)
    cosine, sine_part = phases(bin_index)
    seg_local = whitened.shape[1]
    freq_bins = whitened.shape[2]
    norm_scale = 1.0 / math.sqrt(seg_local * lax.axis_size("seg") * freq_bins)
    rotated = rotate(whitened, cosine, sine_part)
    shard_cols = lax.all_gather(whitened, "sta", axis=3, tiled=True)
    columns = shard_cols.reshape(-1, shard_cols.shape[3])
    product = pair_block(rotated, columns, norm_scale)
    return lax.psum_scatter(product, "seg", scatter_dimension=1, tiled=True).astype(jnp.float32)


def swap(array, axis, flip, senders=None):
    count = lax.axis_size(axis)
    pairs = [(i, i ^ flip) for i in range(count) if senders is None or i in senders]
    return lax.ppermute(array, axis, pairs)


def seg_reduce(tile):
    segs = lax.axis_size("seg")
    me = lax.axis_index("seg")
    lags, blocks, rows, cols = tile.shape
    part = tile.reshape(lags, blocks, segs, rows // segs, cols)
    flip = 1
    while flip < segs:
        mine = (me // flip) % 2
        halves = part.reshape(lags, blocks, part.shape[2] // 2, 2, rows // segs, cols)
        keep = lax.dynamic_index_in_dim(halves, mine, 3, keepdims=False)
        give = lax.dynamic_index_in_dim(halves, 1 - mine, 3, keepdims=False)
        got = swap(give, "seg", flip)
        part = (keep.astype(jnp.float32) + got.astype(jnp.float32)).astype(jnp.bfloat16)
        flip *= 2
    return part[:, :, 0]


def body(spectra, bin_index):
    whitened = whiten(spectra)
    cosine, sine_part = phases(bin_index)
    seg_local, freq_bins, stations = whitened.shape[1:]
    segs = lax.axis_size("seg")
    norm_scale = 1.0 / math.sqrt(seg_local * segs * freq_bins)
    me = lax.axis_index("sta")
    is_end = (me // 2 == 0) | (me // 2 == 3)
    middles = (2, 3, 4, 5)

    def product(rotated, column_block):
        return pair_block(rotated, column_block.reshape(-1, stations), norm_scale)

    def finish(part):
        return part[:, 0], swap(part[:, 1], "sta", 1)

    near = swap(whitened, "sta", 2)
    cross = swap(whitened, "sta", 6, middles)
    beside = swap(whitened, "sta", 1)
    own_rows = rotate(whitened, cosine, sine_part)
    own_own = product(own_rows, whitened)
    near, cross, beside, own_rows, own_own = lax.optimization_barrier(
        (near, cross, beside, own_rows, own_own)
    )

    far_end = swap(cross, "sta", 2, middles)
    far_mid = swap(near, "sta", 6, middles)
    near_beside = swap(near, "sta", 1)
    beside_rows = rotate(beside, cosine, sine_part)
    rows = [own_rows, beside_rows]
    near_rows = rotate(near, cosine, sine_part)

    def tile(row_parts, column_block):
        return seg_reduce(jnp.stack([product(r, column_block) for r in row_parts], axis=1))

    part_own = seg_reduce(jnp.stack([own_own, product(beside_rows, whitened)], axis=1))
    part_near = tile(rows, near)
    part_cross = tile(rows, cross)
    far_end, far_mid, near_beside, near_rows, part_own, part_near, part_cross = (
        lax.optimization_barrier(
            (far_end, far_mid, near_beside, near_rows, part_own, part_near, part_cross)
        )
    )

    far = jnp.where(is_end, far_end, far_mid)
    lent_rows = [near_rows, rotate(near_beside, cosine, sine_part)]
    lent = jnp.stack(finish(tile(lent_rows, far)), axis=1)
    tile_far = finish(tile(rows, far))
    tile_own, tile_near, tile_cross = finish(part_own), finish(part_near), finish(part_cross)
    borrowed = swap(lent, "sta", 2, middles)
    tile_cross = [jnp.where(is_end, borrowed[:, k], tile_cross[k]) for k in range(2)]

    out = jnp.zeros((LAGS, stations // segs, stations * lax.axis_size("sta")), jnp.float32)
    for flip, pair in ((0, tile_own), (2, tile_near), (6, tile_cross), (4, tile_far)):
        for y_flip in range(2):
            column = (me ^ (flip + y_flip)) * stations
            out = lax.dynamic_update_slice_in_dim(
                out, pair[y_flip].astype(jnp.float32), column, axis=2
            )
    return out


def solution(mesh):
    placed = (P(None, "seg", None, "sta"), P())
    chosen = body if mesh.shape["sta"] == 8 else general_body
    return jax.shard_map(
        chosen, mesh=mesh, in_specs=placed, out_specs=P(None, ("sta", "seg"), None), check_vma=False
    )
```
